128 devices in a mesh: col: 4 (over y), blk: 32 (over x, z, core).
Axes of the slice: x: 4, y: 4, z: 4, core: 2. Of those that a mesh axis runs over, the one named last changes fastest.
Arguments:
- corner_up: bfloat16 [4, 256, 256], P('col'), may hold values from -0.375 to 0.375
- corner_dn: bfloat16 [4, 256, 256], P('col'), may hold values from -0.375 to 0.375
- edge_top: bfloat16 [4, 256, 36, 256], P('col', 'blk'), may hold values from -6 to 6
- edge_bot: bfloat16 [4, 256, 36, 256], P('col', 'blk'), may hold values from -6 to 6
- edge_up: bfloat16 [4, 256, 36, 256], P('col', 'blk'), may hold values from -0.375 to 0.375
- edge_dn: bfloat16 [4, 256, 36, 256], P('col', 'blk'), may hold values from -0.375 to 0.375
- site_up: bfloat16 [4, 36, 36, 36, 36], P('col'), may hold values from -0.15625 to 0.15625
- site_dn: bfloat16 [4, 36, 36, 36, 36], P('col'), may hold values from -0.15625 to 0.15625
- proj_up: bfloat16 [4, 9216, 256], P('col', 'blk'), may hold values from -0.0625 to 0.0625
- proj_dn: bfloat16 [4, 9216, 256], P('col', 'blk'), may hold values from -0.0625 to 0.0625
Outputs:
- half_proj: bfloat16 [4, 9216, 256], P('col', 'blk')
- next_up: bfloat16 [4, 256, 256], P('col', 'blk')
- next_dn: bfloat16 [4, 256, 256], P('col', 'blk')
The draws below stay inside these ranges and needn't reach their ends.
All inputs are finite; a program needn't handle non-finite values.
Results may differ from the reference program's by a relative error of at most 0.018.
Values may be sent and summed in bfloat16 or wider, within the bound.
A program may use at most 128 MiB of HBM per device.

```python
import jax
import jax.numpy as jnp
from jax import lax

CHI = 256
D2 = 36
COLS = 4


def steps_of(rng, dims, cuts, low, largest):
    level = 1.0
    for position, parts in cuts:
        steps = jax.random.uniform(jax.random.fold_in(jax.random.fold_in(rng, 6), position), (parts,), jnp.float32, low / len(cuts), largest / len(cuts))
        level = level * jnp.repeat(jnp.exp(steps), dims[position] // parts).reshape((-1,) + (1,) * (len(dims) - 1 - position))
    return level


def normal_values(stream_key, extent, deviation, bound, pieces=(), dtype=jnp.bfloat16):
    drawn = deviation * jax.random.normal(stream_key, extent, jnp.float32)
    if pieces:
        drawn = drawn * steps_of(stream_key, extent, pieces, -0.22, 0.18)
    return jnp.clip(drawn, -bound, bound).astype(dtype)


def setup_inputs(seed: int = 0) -> dict:
    key_list = jax.random.split(jax.random.key(seed), 11)
    corner_up = normal_values(key_list[0], (COLS, CHI, CHI), CHI ** -0.5, 0.375, ((0, 4),))
    corner_dn = normal_values(key_list[1], (COLS, CHI, CHI), CHI ** -0.5, 0.375, ((0, 4),))
    edge_top = normal_values(key_list[2], (COLS, CHI, D2, CHI), 1.0, 6.0, ((0, 4), (1, 32)))
    edge_bot = normal_values(key_list[3], (COLS, CHI, D2, CHI), 1.0, 6.0, ((0, 4), (1, 32)))
    edge_up = normal_values(key_list[4], (COLS, CHI, D2, CHI), CHI ** -0.5, 0.375, ((0, 4), (1, 32)))
    edge_dn = normal_values(key_list[5], (COLS, CHI, D2, CHI), CHI ** -0.5, 0.375, ((0, 4), (1, 32)))
    site_up = normal_values(key_list[6], (COLS, D2, D2, D2, D2), (D2 * D2) ** -0.5, 0.15625, ((0, 4),))
    site_dn = normal_values(key_list[7], (COLS, D2, D2, D2, D2), (D2 * D2) ** -0.5, 0.15625, ((0, 4),))
    proj_up = normal_values(key_list[8], (COLS, CHI * D2, CHI), (CHI * D2) ** -0.5, 0.0625, ((0, 4), (1, 32)))
    proj_dn = normal_values(key_list[9], (COLS, CHI * D2, CHI), (CHI * D2) ** -0.5, 0.0625, ((0, 4), (1, 32)))
    return {"corner_up": corner_up, "corner_dn": corner_dn, "edge_top": edge_top, "edge_bot": edge_bot, "edge_up": edge_up, "edge_dn": edge_dn, "site_up": site_up, "site_dn": site_dn, "proj_up": proj_up, "proj_dn": proj_dn}


def enlarge(edge, grown, site):
    rows = edge.shape[0]
    wide = jnp.dot(edge.reshape(rows * D2, CHI), grown, preferred_element_type=jnp.float32).astype(jnp.bfloat16)
    wide = wide.reshape(rows, D2 * D2, CHI)
    table = site.transpose(2, 1, 3, 0).reshape(D2 * D2, D2 * D2)
    block = jnp.einsum("ab,ibj->iaj", table.astype(jnp.float32), wide.astype(jnp.float32)).astype(jnp.bfloat16)
    return block.reshape(rows * D2, D2 * CHI)


def column(items):
    c_up, c_dn, top, bot, e_up, e_dn, s_up, s_dn, p_up, p_dn = items
    grown_up = jnp.dot(c_up, top.reshape(CHI, D2 * CHI), preferred_element_type=jnp.float32).astype(jnp.bfloat16)
    grown_dn = jnp.dot(c_dn, bot.reshape(CHI, D2 * CHI), preferred_element_type=jnp.float32).astype(jnp.bfloat16)
    quad_up = enlarge(e_up, grown_up, s_up)
    quad_dn = enlarge(e_dn, grown_dn, s_dn)
    cut = lax.dot_general(quad_dn, p_dn, (((0,), (0,)), ((), ())), preferred_element_type=jnp.float32).astype(jnp.bfloat16)
    half = jnp.dot(quad_up, cut, preferred_element_type=jnp.float32) * (1.0 / (CHI * D2) ** 0.5)
    fresh_up = lax.dot_general(p_up, grown_up.reshape(CHI * D2, CHI), (((0,), (0,)), ((), ())), preferred_element_type=jnp.float32).astype(jnp.bfloat16)
    fresh_dn = lax.dot_general(p_dn, grown_dn.reshape(CHI * D2, CHI), (((0,), (0,)), ((), ())), preferred_element_type=jnp.float32).astype(jnp.bfloat16)
    return half.astype(jnp.bfloat16), fresh_up, fresh_dn


def reference(corner_up, corner_dn, edge_top, edge_bot, edge_up, edge_dn, site_up, site_dn, proj_up, proj_dn):
    half_proj, fresh_up, fresh_dn = lax.map(column, (corner_up, corner_dn, edge_top, edge_bot, edge_up, edge_dn, site_up, site_dn, proj_up, proj_dn))
    return half_proj, jnp.roll(fresh_up, 1, axis=0), jnp.roll(fresh_dn, 1, axis=0)
```

```python
import functools

import jax
import jax.numpy as jnp
from jax import lax
from jax.experimental import pallas as pl
from jax.experimental.pallas import tpu as pltpu
from jax.sharding import PartitionSpec as P

MESH = pl.DeviceIdType.MESH
BF = jnp.bfloat16
F32 = jnp.float32

CHI = 256
D = 36
DP = 40
NX = 4
NZ = 4
JW = 64
NU = 18
KT = 1536
TCH = 3
TROWS = 12 * DP
CW = 12 * JW


def low_lanes(shape):
    return lax.broadcasted_iota(jnp.int32, shape, len(shape) - 1) < 64


def swap_halves(a, b):
    low = low_lanes(a.shape)
    ra = pltpu.roll(a, 64, a.ndim - 1)
    rb = pltpu.roll(b, 64, b.ndim - 1)
    return jnp.where(low, a, rb), jnp.where(low, ra, b)


def kernel(
    cu, cd, et, eb, eu, ed, su, sd, pu, pd,
    half_out, nu_out, nd_out,
    send_e, e_all, rows, grown, grown_f, rows_f, table, stg, wk, qt, pt, p2,
    cp, cs, cb, cx, cf, hs, hr, fs, fr, fw, fn,
    stg_sem, ez_s, ez_r, ex_s, ex_r, eo_s, eo_r, rz_s, rz_r,
    c1_s, c1_r, c2_s, c2_r, c3_s, c3_r, c4_s, c4_r, h_s, h_r, f1_s, f1_r, f2_s, f2_r,
):
    col = lax.axis_index("col")
    blk = lax.axis_index("blk")
    x = blk // 8
    z = (blk // 2) % 4
    c = blk % 2
    cols = lax.axis_size("col")

    def dev(x_, z_, c_, col_=None):
        return (col if col_ is None else col_, (x_ * 4 + z_) * 2 + c_)

    def mod4(v):
        return (v + 8) % 4

    def rcopy(src, dst, ssem, rsem, device):
        return pltpu.make_async_remote_copy(
            src_ref=src, dst_ref=dst, send_sem=ssem, recv_sem=rsem, device_id=device, device_id_type=MESH
        )

    oc = 1 - c
    xp = [mod4(x + s) for s in range(4)]
    xm = [mod4(x - s) for s in range(4)]
    zp = [mod4(z + s) for s in range(4)]
    zm = [mod4(z - s) for s in range(4)]
    cnext = (col + 1) % cols
    cprev = (col + cols - 1) % cols

    sites = (sd, su)
    steps = [(k, q) for k in range(2) for q in range(6)]

    def site_copy(n):
        k, q = steps[n]
        return pltpu.make_async_copy(sites[k].at[pl.ds(6 * q, 6)], stg.at[n % 2], stg_sem.at[n % 2])

    site_copy(0).start()
    site_copy(1).start()

    bar = pltpu.get_barrier_semaphore()
    peers = [dev(x, z, oc)]
    for s in (1, 2, 3):
        peers += [dev(xp[s], z, c), dev(xp[s], z, oc), dev(x, zp[s], c)]
    for p_ in peers + [dev(x, z_, c, cprev) for z_ in range(4)]:
        pl.semaphore_signal(bar, inc=1, device_id=p_, device_id_type=MESH)

    for k, src in enumerate((eb, et)):
        v = src[...].astype(F32).reshape(NU, 2, 8, CHI)
        for h in range(2):
            a = v[:, 0, :, 128 * h : 128 * h + 128].reshape(NU * 8, 128)
            b = v[:, 1, :, 128 * h : 128 * h + 128].reshape(NU * 8, 128)
            lo, hi = swap_halves(a, b)
            send_e[k, 2 * h] = lo.astype(BF).reshape(NU, 8, 128)
            send_e[k, 2 * h + 1] = hi.astype(BF).reshape(NU, 8, 128)
        e_all[k, x, c, z] = send_e[k, z]

    zero4 = jnp.zeros((DP - D, CHI), F32)
    for kind, src in enumerate((ed, pd, eu, pu)):
        v = src[...].astype(F32)
        if kind % 2 == 0:
            v = v.reshape(8 * D, CHI)
        for h in range(2):
            rows_f[h, 0 : 8 * D] = v[:, 128 * h : 128 * h + 128]
        for i in range(8):
            at = pl.ds(i, D, stride=8) if kind % 2 == 0 else pl.ds(D * i, D)
            piece = jnp.concatenate([rows_f[h, at, :] for h in range(2)], axis=1)
            rows[kind, z, i] = jnp.concatenate([piece, zero4], axis=0).astype(BF)

    pl.semaphore_wait(bar, 14)

    def ez(k, s):
        return rcopy(send_e.at[k, zp[s]], e_all.at[k, x, c, z], ez_s.at[k, s], ez_r.at[k, s], dev(x, zp[s], c))

    def ez_in(k, s):
        return rcopy(send_e.at[k, zm[s]], e_all.at[k, x, c, zm[s]], ez_s.at[k, s], ez_r.at[k, s], dev(x, zm[s], c))

    def rz(kind, s):
        return rcopy(rows.at[kind, z], rows.at[kind, z], rz_s.at[kind, s], rz_r.at[kind, s], dev(x, zp[s], c))

    def rz_in(kind, s):
        return rcopy(rows.at[kind, zm[s]], rows.at[kind, zm[s]], rz_s.at[kind, s], rz_r.at[kind, s], dev(x, zm[s], c))

    for k in range(2):
        for s in (1, 3, 2):
            ez(k, s).start()
    for kind in range(4):
        for s in (1, 3, 2):
            rz(kind, s).start()

    def make_table(n):
        k, q = steps[n]
        site_copy(n).wait()

        def body(tp, carry):
            row = pl.multiple_of(80 * tp, 16)
            for h in range(2):
                parts = []
                for t in range(2):
                    v = [stg[n % 2, 3 * h + w, 2 * tp + t].astype(F32) for w in range(3)]
                    gap = jnp.zeros((D, 4), F32)
                    wide = jnp.concatenate([v[0], gap, v[1], gap, v[2], jnp.zeros((D, 12), F32)], axis=1)
                    parts += [wide, jnp.zeros((4, 128), F32)]
                table[k, pl.ds(row, 80), 256 * q + 128 * h : 256 * q + 128 * h + 128] = jnp.concatenate(
                    parts, axis=0
                ).astype(BF)
            return carry

        lax.fori_loop(0, 18, body, 0)
        if n + 2 < len(steps):
            site_copy(n + 2).start()

    def ex(k, s):
        ref = e_all.at[k, x, c]
        return rcopy(ref, ref, ex_s.at[k, s], ex_r.at[k, s], dev(xp[s], z, c))

    def ex_in(k, s):
        ref = e_all.at[k, xm[s], c]
        return rcopy(ref, ref, ex_s.at[k, s], ex_r.at[k, s], dev(xm[s], z, c))

    def eo(k, s):
        ref = e_all.at[k, xm[s], c]
        return rcopy(ref, ref, eo_s.at[k, s], eo_r.at[k, s], dev(x, z, oc))

    def eo_in(k, s):
        ref = e_all.at[k, xm[s], oc]
        return rcopy(ref, ref, eo_s.at[k, s], eo_r.at[k, s], dev(x, z, oc))

    make_table(0)
    make_table(1)
    for k in range(2):
        for s in (1, 3, 2):
            ez_in(k, s).wait_recv()
        for s in (1, 3, 2):
            ex(k, s).start()
        eo(k, 0).start()
    for n in range(2, 9):
        make_table(n)
    for s in (1, 3, 2):
        ex_in(0, s).wait_recv()
        eo(0, s).start()
    for n in range(9, 12):
        make_table(n)
    for s in (0, 1, 3, 2):
        eo_in(0, s).wait_recv()

    def grow(k, corner):
        cv = corner[...]

        def body(m, carry):
            halves = []
            for w in range(2):
                parts = [
                    e_all[k, x_, c_, z_, 2 * m + w].astype(F32) for x_ in range(4) for z_ in range(4) for c_ in range(2)
                ]
                halves.append(jnp.concatenate(parts, axis=0))
            e = jnp.concatenate(halves, axis=1).astype(BF)
            g = jnp.dot(cv, e, preferred_element_type=F32)
            grown_f[:, pl.ds(pl.multiple_of(256 * m, 256), 256)] = g
            grown[:, pl.ds(pl.multiple_of(256 * m, 256), 256)] = g.astype(BF)
            return carry

        lax.fori_loop(0, 9, body, 0)

    def fresh(k):
        kind = 1 + 2 * k
        v = rows[kind].astype(F32).reshape(32 * DP, CHI)
        for h in range(2):
            rows_f[h] = v[:, 128 * h : 128 * h + 128]
        gparts = []
        for u in range(D):
            for h in range(2):
                p2[32 * u : 32 * u + 32, 128 * h : 128 * h + 128] = rows_f[h, pl.ds(u, 32, stride=DP), :].astype(BF)
        for m in range(NU):
            g = jnp.concatenate(
                [
                    grown_f[pl.ds(pl.multiple_of(64 * x + 16 * z_ + 8 * c, 8), 8), 128 * m : 128 * m + 128]
                    for z_ in range(4)
                ],
                axis=0,
            )
            gparts += [g, pltpu.roll(g, 64, 1)]
        g2 = jnp.concatenate(gparts, axis=0).astype(BF)
        return lax.dot_general(p2[...], g2, (((0,), (0,)), ((), ())), preferred_element_type=F32)

    def widen(k):
        kind = 2 * k

        def body(g, carry):
            left = rows[kind, g // 2, pl.ds(4 * (g % 2), 4)].astype(F32).reshape(4 * DP, CHI).astype(BF)
            for qq in range(3):
                w = jnp.dot(left, grown[:, 768 * qq : 768 * qq + 768], preferred_element_type=F32)
                for ip in range(2):
                    us = []
                    for m in range(6):
                        a = w[80 * ip : 80 * ip + 40, 128 * m : 128 * m + 128]
                        b = w[80 * ip + 40 : 80 * ip + 80, 128 * m : 128 * m + 128]
                        us += list(swap_halves(a, b))
                    for h in range(4):
                        blockv = jnp.concatenate(us[3 * h : 3 * h + 3] + [jnp.zeros((8, 128), F32)], axis=0)
                        row = 512 * qq + 128 * h
                        wk[g, row : row + 128, 128 * ip : 128 * ip + 128] = blockv.astype(BF)
            return carry

        lax.fori_loop(0, 8, body, 0)

    def quad(k, ch):
        def body(g, carry):
            qv = jnp.dot(
                table[k, TROWS * ch : TROWS * ch + TROWS, :], wk[g], preferred_element_type=F32
            )
            for tp in range(6):
                for ip in range(2):
                    a = qv[80 * tp : 80 * tp + 40, 128 * ip : 128 * ip + 128]
                    b = qv[80 * tp + 40 : 80 * tp + 80, 128 * ip : 128 * ip + 128]
                    o0, o1 = swap_halves(a, b)
                    lane = CW * ch + 128 * tp
                    qt[pl.ds(pl.multiple_of(160 * g + 80 * ip, 16), 80), lane : lane + 128] = jnp.concatenate(
                        [o0, o1], axis=0
                    ).astype(BF)
            return carry

        lax.fori_loop(0, 8, body, 0)

    grow(0, cd)
    for s in (1, 3, 2):
        rz_in(0, s).wait_recv()
    for s in (1, 3, 2):
        rz_in(1, s).wait_recv()
    fresh_dn = fresh(0)
    fw[...] = fresh_dn
    for h in range(2):
        pt[128 * h : 128 * h + 128, :] = rows_f[h].T.astype(BF)
    widen(0)
    for s in (1, 3, 2):
        ex_in(1, s).wait_recv()
        eo(1, s).start()

    def c1(ch):
        return rcopy(cp.at[ch, oc], cs.at[ch], c1_s.at[ch], c1_r.at[ch], dev(x, z, oc))

    def c2(ch, s):
        return rcopy(cb.at[ch, xp[s]], cx.at[ch, s], c2_s.at[ch, s], c2_r.at[ch, s], dev(xp[s], z, c))

    def c3(ch, s):
        ref = cf.at[ch, c, x]
        return rcopy(ref, ref, c3_s.at[ch, s], c3_r.at[ch, s], dev(xp[s], z, c))

    def c3_in(ch, s):
        ref = cf.at[ch, c, xm[s]]
        return rcopy(ref, ref, c3_s.at[ch, s], c3_r.at[ch, s], dev(xm[s], z, c))

    def c4(ch):
        ref = cf.at[ch, c]
        return rcopy(ref, ref, c4_s.at[ch], c4_r.at[ch], dev(x, z, oc))

    def c4_in(ch):
        ref = cf.at[ch, oc]
        return rcopy(ref, ref, c4_s.at[ch], c4_r.at[ch], dev(x, z, oc))

    def cut1(ch):
        part = jnp.dot(pt[...], qt[:, CW * ch : CW * ch + CW], preferred_element_type=F32).astype(BF)
        cp[ch] = part.reshape(2, 128, CW)
        c1(ch).start()

    def cut2(ch):
        c1(ch).wait_recv()
        both = cp[ch, c].astype(F32) + cs[ch].astype(F32)
        cb[ch] = both.astype(BF).reshape(4, 32, CW)
        for s in (1, 3, 2):
            c2(ch, s).start()

    def cut3(ch):
        for s in (1, 3, 2):
            c2(ch, s).wait_recv()
        total = cb[ch, x].astype(F32)
        for s in (1, 2, 3):
            total = total + cx[ch, s].astype(F32)
        cf[ch, c, x] = total.astype(BF)
        for s in (1, 3, 2):
            c3(ch, s).start()

    def cut4(ch):
        for s in (1, 3, 2):
            c3_in(ch, s).wait_recv()
        c4(ch).start()

    quad(0, 0)
    cut1(0)
    quad(0, 1)
    cut1(1)
    cut2(0)
    quad(0, 2)
    cut1(2)
    cut2(1)
    cut3(0)

    for s in (0, 1, 3, 2):
        eo_in(1, s).wait_recv()
    grow(1, cu)
    for s in (1, 3, 2):
        rz_in(3, s).wait_recv()
    fresh_up = fresh(1)
    both = jnp.where(low_lanes((CHI, 128)), fw[...], pltpu.roll(fresh_up, 64, 1))
    for x_ in range(4):
        for z_ in range(4):
            for c_ in range(2):
                at = 64 * x_ + 16 * z_ + 8 * c_
                fs[2 * x_ + c_, z_] = both[at : at + 8]
    me = 2 * x + c

    def f1_pairs():
        out = []
        for s in range(4):
            for o in range(2):
                if s or o:
                    out.append((2 * s + o, 2 * xp[s] + (oc if o else c), dev(xp[s], z, oc if o else c)))
        return out

    def f1(n, to, device):
        return rcopy(fs.at[to], fr.at[n], f1_s.at[n], f1_r.at[n], device)

    for a in f1_pairs():
        f1(*a).start()
    cut2(2)
    cut3(1)
    for s in (1, 3, 2):
        rz_in(2, s).wait_recv()
    widen(1)
    cut3(2)
    cut4(0)
    quad(1, 0)
    cut4(1)

    def f2(z_):
        return rcopy(fr.at[0, z_], fn.at[z], f2_s.at[z_], f2_r.at[z], dev(x, z_, c, cnext))

    def f2_in(z_):
        return rcopy(fr.at[0, z_], fn.at[z_], f2_s.at[z_], f2_r.at[z_], dev(x, z_, c, cnext))

    for a in f1_pairs():
        f1(*a).wait_recv()
    total = fs[me]
    for n in range(1, 8):
        total = total + fr[n]
    fr[0] = total
    for z_ in range(4):
        f2(z_).start()
    quad(1, 1)
    cut4(2)
    quad(1, 2)

    for ch in range(TCH):
        c4_in(ch).wait_recv()

    def h1(s):
        return rcopy(hs.at[zp[s]], hr.at[s], h_s.at[s], h_r.at[s], dev(x, zp[s], c))

    scale = 1.0 / (CHI * D) ** 0.5

    def half_of(z_):
        acc = None
        for ch in range(TCH):
            left = qt[pl.ds(pl.multiple_of(320 * z_, 320), 320), CW * ch : CW * ch + CW]
            right = cf[ch].reshape(CHI, CW)
            t = lax.dot_general(left, right, (((1,), (1,)), ((), ())), preferred_element_type=F32)
            acc = t if acc is None else acc + t
        return acc * scale

    for s in (2, 1, 3):
        hs[zp[s]] = half_of(zp[s]).astype(BF)
        h1(s).start()
    acc = half_of(z)
    for z_ in range(4):
        f2_in(z_).wait_recv()
    lo, hi = swap_halves(fn[0], fn[1])
    lo2, hi2 = swap_halves(fn[2], fn[3])
    nd_out[:, 0:128] = lo.astype(BF)
    nd_out[:, 128:256] = lo2.astype(BF)
    nu_out[:, 0:128] = hi.astype(BF)
    nu_out[:, 128:256] = hi2.astype(BF)
    for s in (1, 3, 2):
        h1(s).wait_recv()
        acc = acc + hr[s].astype(F32)
    half_out[...] = acc.reshape(8, DP, CHI)[:, :D].astype(BF)

    for k in range(2):
        for s in (1, 2, 3):
            ez(k, s).wait_send()
            ex(k, s).wait_send()
        for s in range(4):
            eo(k, s).wait_send()
    for kind in range(4):
        for s in (1, 2, 3):
            rz(kind, s).wait_send()
    for ch in range(TCH):
        c1(ch).wait_send()
        for s in (1, 2, 3):
            c2(ch, s).wait_send()
            c3(ch, s).wait_send()
        c4(ch).wait_send()
    for s in (1, 2, 3):
        h1(s).wait_send()
    for a in f1_pairs():
        f1(*a).wait_send()
    for z_ in range(4):
        f2(z_).wait_send()


def per_device(cu, cd, et, eb, eu, ed, su, sd, pu, pd):
    vmem = pl.BlockSpec(memory_space=pltpu.VMEM)
    hbm = pl.BlockSpec(memory_space=pl.ANY)
    dma = pltpu.SemaphoreType.DMA
    scratch = [
        pltpu.VMEM((2, 4, NU, 8, 128), BF),
        pltpu.VMEM((2, 4, 2, 4, NU, 8, 128), BF),
        pltpu.VMEM((4, 4, 8, DP, CHI), BF),
        pltpu.VMEM((CHI, D * JW), BF),
        pltpu.VMEM((CHI, D * JW), F32),
        pltpu.VMEM((2, 32 * DP, 128), F32),
        pltpu.VMEM((2, D * DP, KT), BF),
        pltpu.VMEM((2, 6, D, D, D), BF),
        pltpu.VMEM((8, KT, 256), BF),
        pltpu.VMEM((32 * DP, D * JW), BF),
        pltpu.VMEM((CHI, 32 * DP), BF),
        pltpu.VMEM((D * 32, CHI), BF),
        pltpu.VMEM((TCH, 2, 128, CW), BF),
        pltpu.VMEM((TCH, 128, CW), BF),
        pltpu.VMEM((TCH, 4, 32, CW), BF),
        pltpu.VMEM((TCH, 4, 32, CW), BF),
        pltpu.VMEM((TCH, 2, 4, 32, CW), BF),
        pltpu.VMEM((4, 8 * DP, CHI), BF),
        pltpu.VMEM((4, 8 * DP, CHI), BF),
        pltpu.VMEM((8, 4, 8, 128), F32),
        pltpu.VMEM((8, 4, 8, 128), F32),
        pltpu.VMEM((CHI, 128), F32),
        pltpu.VMEM((4, 8, 128), F32),
        dma((2,)),
        dma((2, 4)), dma((2, 4)),
        dma((2, 4)), dma((2, 4)),
        dma((2, 4)), dma((2, 4)),
        dma((4, 4)), dma((4, 4)),
        dma((TCH,)), dma((TCH,)),
        dma((TCH, 4)), dma((TCH, 4)),
        dma((TCH, 4)), dma((TCH, 4)),
        dma((TCH,)), dma((TCH,)),
        dma((4,)), dma((4,)),
        dma((8,)), dma((8,)),
        dma((4,)), dma((4,)),
    ]
    swap = lambda e: jnp.transpose(e[0], (1, 0, 2))
    half, nu, nd = pl.pallas_call(
        kernel,
        out_shape=(
            jax.ShapeDtypeStruct((8, D, CHI), BF),
            jax.ShapeDtypeStruct((8, CHI), BF),
            jax.ShapeDtypeStruct((8, CHI), BF),
        ),
        in_specs=[vmem] * 6 + [hbm] * 2 + [vmem] * 2,
        out_specs=(vmem,) * 3,
        scratch_shapes=scratch,
        compiler_params=pltpu.CompilerParams(
            collective_id=0, has_side_effects=True, vmem_limit_bytes=62 * 1024 * 1024
        ),
        name="ctm_step",
    )(cu[0], cd[0], swap(et), swap(eb), swap(eu), swap(ed), su[0], sd[0], pu[0], pd[0])
    return half.reshape(1, 8 * D, CHI), nu[None], nd[None]


def solution(mesh):
    in_specs = (
        P("col", None, None),
        P("col", None, None),
        P("col", "blk", None, None),
        P("col", "blk", None, None),
        P("col", "blk", None, None),
        P("col", "blk", None, None),
        P("col", None, None, None, None),
        P("col", None, None, None, None),
        P("col", "blk", None),
        P("col", "blk", None),
    )
    out_specs = (P("col", "blk", None), P("col", "blk", None), P("col", "blk", None))
    return jax.shard_map(
        per_device, mesh=mesh, in_specs=in_specs, out_specs=out_specs, check_vma=False
    )
```
